64 devices in a mesh: rep: 8 (over x, y, core), dp: 8 (over z).
Axes of the slice: x: 2, y: 2, z: 8, core: 2. Of those that a mesh axis runs over, the one named last changes fastest.
The devices are a block of a 4x4x8 slice.
Arguments:
- a: bfloat16 [64, 4, 4096, 768], P(('rep', 'dp')), parts along dimension 0
- g: bfloat16 [64, 4, 4096, 2048], P(('rep', 'dp')), parts along dimension 0
Outputs:
- output: bfloat16 [32, 768, 2048], P('rep'), parts along dimension 0
There are 8 independent parts. The reference program is written for one: setup_inputs(seed, part) draws one part's arguments, and reference() takes and returns one part's arrays. A program takes and returns all parts, laid end to end along the dimension named above; each array names one.
All inputs are finite; a program needn't handle non-finite values.
Results may differ from the reference program's by a relative error of at most 0.012.
Values are sent between devices in bfloat16 or wider.
A program may use at most 768 MiB of HBM per device.

```python
import jax
import jax.numpy as jnp
from jax import lax

DEVICES = 8
MATRICES = 4
TOKENS = 4096
D = 768
FF = 2048


def setup_inputs(seed: int = 0, part: int = 0) -> dict:
    ka, kg, ks = (jax.random.fold_in(k, part) for k in jax.random.split(jax.random.key(seed), 3))
    size = 2.0 ** jax.random.uniform(ks, (DEVICES, MATRICES, 1, 1), jnp.float32, -1.0, 1.0)
    a = jax.random.normal(ka, (DEVICES, MATRICES, TOKENS, D), jnp.float32)
    g = size * jax.random.normal(kg, (DEVICES, MATRICES, TOKENS, FF), jnp.float32) * (DEVICES * TOKENS) ** -0.5
    return {"a": a.astype(jnp.bfloat16), "g": g.astype(jnp.bfloat16)}


def reference(a, g):
    def take(so_far, one):
        return so_far + jnp.einsum("ntd,ntf->ndf", *one, preferred_element_type=jnp.float32), None

    return lax.scan(take, jnp.zeros((MATRICES, D, FF), jnp.float32), (a, g))[0].astype(jnp.bfloat16)
```

```python
import functools

import jax
import jax.numpy as jnp
from jax import lax
from jax.experimental import pallas as pl
from jax.experimental.pallas import tpu as pltpu
from jax.sharding import PartitionSpec as P

MESH = pl.DeviceIdType.MESH
SLOTS = 4


def kernel(n, a_hbm, g_hbm, out_hbm, a_v, g_v, part, held, done, a_sem, g_sem, send_sem, recv_sem, out_sem):
    matrices, halves, _, rows, cols = held.shape
    me = lax.axis_index("dp")
    peers = (lax.rem(me + 1, n), lax.rem(me + n - 1, n))

    def block(h, s):
        return lax.rem(me + n + n - 1 - s, n) if h == 0 else lax.rem(me + 1 + s, n)

    def load_a(m, h):
        return pltpu.make_async_copy(a_hbm.at[0, m, :, pl.ds(h * rows, rows)], a_v.at[m, h], a_sem.at[m, h])

    def load_g(i, h):
        b = pl.multiple_of(block(h, lax.div(i, matrices)) * cols, cols)
        slot = lax.rem(2 * i + h, SLOTS)
        return pltpu.make_async_copy(g_hbm.at[0, lax.rem(i, matrices), :, pl.ds(b, cols)], g_v.at[slot], g_sem.at[slot])

    def hop(buf, phase, m, h, s, b):
        at = ((phase * n + s) * matrices + m) * halves + h
        return pltpu.make_async_remote_copy(
            src_ref=buf.at[m, h, b], dst_ref=buf.at[m, h, b], send_sem=send_sem.at[at], recv_sem=recv_sem.at[at],
            device_id={"dp": peers[h]}, device_id_type=MESH,
        )

    def put(m, h, b):
        return pltpu.make_async_copy(
            done.at[m, h, b],
            out_hbm.at[m, pl.ds(h * rows, rows), pl.ds(pl.multiple_of(b * cols, cols), cols)],
            out_sem.at[(m * halves + h) * n + b],
        )

    items = n * matrices

    def term(i, m, h):
        load_g(i, h).wait()
        part[...] = lax.dot_general(
            a_v[m, h], g_v[lax.rem(2 * i + h, SLOTS)], (((0,), (0,)), ((), ())), preferred_element_type=jnp.float32
        )

        @pl.when(i + SLOTS // 2 < items)
        def _():
            load_g(i + SLOTS // 2, h).start()

    for h in range(halves):
        load_a(0, h).start()
        load_g(0, h).start()
    for h in range(halves):
        load_g(1, h).start()
    barrier = pltpu.get_barrier_semaphore()
    for p in peers:
        pl.semaphore_signal(barrier, inc=1, device_id={"dp": p}, device_id_type=MESH)
    pl.semaphore_wait(barrier, 2)

    def first(m, c):
        for h in range(halves):
            @pl.when(m + 1 < matrices)
            def _():
                load_a(m + 1, h).start()

            load_a(m, h).wait()
            term(m, m, h)
            b = block(h, 0)
            held[m, h, b] = part[...].astype(held.dtype)
            hop(held, 0, m, h, 0, b).start()
        return c

    lax.fori_loop(0, matrices, first, 0)

    def middle(i, c):
        m, s = lax.rem(i, matrices), lax.div(i, matrices)
        for h in range(halves):
            term(i, m, h)
            b = block(h, s)
            hop(held, 0, m, h, s - 1, b).wait_recv()
            held[m, h, b] = (part[...] + held[m, h, b].astype(jnp.float32)).astype(held.dtype)
            hop(held, 0, m, h, s, b).start()
        return c

    lax.fori_loop(matrices, items - matrices, middle, 0)

    def last(m, c):
        i = items - matrices + m
        for h in range(halves):
            term(i, m, h)
            hop(held, 0, m, h, n - 2, me).wait_recv()
            done[m, h, me] = (part[...] + held[m, h, me].astype(jnp.float32)).astype(done.dtype)
            hop(done, 1, m, h, 0, me).start()
            put(m, h, me).start()
        return c

    lax.fori_loop(0, matrices, last, 0)

    def gather(i, c):
        m, s = lax.rem(i, matrices), lax.div(i, matrices) + 1
        for h in range(halves):
            b = lax.rem(me + n - s, n) if h == 0 else lax.rem(me + s, n)
            hop(done, 1, m, h, s - 1, b).wait_recv()

            @pl.when(s < n - 1)
            def _():
                hop(done, 1, m, h, s, b).start()

            put(m, h, b).start()
        return c

    lax.fori_loop(0, items - matrices, gather, 0)

    def drain(i, c):
        m, s = lax.rem(i, matrices), lax.div(i, matrices)
        for h in range(halves):
            hop(held, 0, m, h, s, me).wait_send()
            hop(done, 1, m, h, s, me).wait_send()
            put(m, h, s).wait()
        return c

    lax.fori_loop(0, items - matrices, drain, 0)
    for m in range(matrices):
        for h in range(halves):
            put(m, h, n - 1).wait()


def solution(mesh):
    n = mesh.shape["dp"]

    def step(a, g):
        _, matrices, tokens, d = a.shape
        ff = g.shape[3]
        rows, cols = d // 2, ff // n
        blocks = (matrices, 2, n, rows, cols)
        return pl.pallas_call(
            functools.partial(kernel, n),
            out_shape=jax.ShapeDtypeStruct((matrices, d, ff), jnp.bfloat16),
            in_specs=[pl.BlockSpec(memory_space=pl.ANY)] * 2,
            out_specs=pl.BlockSpec(memory_space=pl.ANY),
            scratch_shapes=[
                pltpu.VMEM((matrices, 2, tokens, rows), jnp.bfloat16),
                pltpu.VMEM((SLOTS, tokens, cols), jnp.bfloat16),
                pltpu.VMEM((rows, cols), jnp.float32),
                pltpu.VMEM(blocks, jnp.bfloat16),
                pltpu.VMEM(blocks, jnp.bfloat16),
                pltpu.SemaphoreType.DMA((matrices, 2)),
                pltpu.SemaphoreType.DMA((SLOTS,)),
                pltpu.SemaphoreType.DMA((2 * n * matrices * 2,)),
                pltpu.SemaphoreType.DMA((2 * n * matrices * 2,)),
                pltpu.SemaphoreType.DMA((matrices * 2 * n,)),
            ],
            compiler_params=pltpu.CompilerParams(
                collective_id=0, has_side_effects=True, vmem_limit_bytes=67043328
            ),
            cost_estimate=pl.CostEstimate(
                flops=2 * matrices * tokens * d * ff, bytes_accessed=2 * matrices * (tokens + d) * (d + ff), transcendentals=0
            ),
        )(a, g)

    return jax.shard_map(
        step, mesh=mesh, in_specs=(P(("rep", "dp")), P(("rep", "dp"))), out_specs=P("rep"), check_vma=False
    )
```

```python
import functools

import jax
import jax.numpy as jnp
from jax import lax
from jax.experimental import pallas as pl
from jax.experimental.pallas import tpu as pltpu
from jax.sharding import PartitionSpec as P

MESH = pl.DeviceIdType.MESH
RINGS = 2
SLOTS = 4
STRIPS = ((0, 128), (128, 256), (384, 384))


def kernel(n, a_hbm, g_hbm, out, a_v, g_v, part, held, a_sem, g_sem, send_sem, recv_sem):
    matrices, _, rows, cols = held.shape
    me = lax.axis_index("dp")
    items = n * matrices

    def way(m):
        return 2 * lax.rem(m, RINGS) - 1

    def block(m, s):
        return lax.rem(me + 2 * n + way(m) * (1 + s), n)

    def tile(b):
        return pl.ds(pl.multiple_of(b * cols, cols), cols)

    def load_a(m, k):
        strip = pl.ds(*STRIPS[k])
        return pltpu.make_async_copy(
            a_hbm.at[0, m, :, strip], a_v.at[m, :, strip], a_sem.at[m * len(STRIPS) + k]
        )

    def load_g(i):
        m, slot = lax.rem(i, matrices), lax.rem(i, SLOTS)
        return pltpu.make_async_copy(g_hbm.at[0, m, :, tile(block(m, lax.div(i, matrices)))], g_v.at[slot], g_sem.at[slot])

    def dot(a, i):
        return lax.dot_general(
            a, g_v[lax.rem(i, SLOTS)], (((0,), (0,)), ((), ())), preferred_element_type=jnp.float32
        )

    def hop(phase, m, s, b, strip=None):
        at = (phase * n + s) * matrices + m
        if phase:
            ref = out.at[m, :, tile(b)]
        else:
            ref = held.at[m, b] if strip is None else held.at[m, b, pl.ds(*strip)]
        return pltpu.make_async_remote_copy(
            src_ref=ref, dst_ref=ref, send_sem=send_sem.at[at], recv_sem=recv_sem.at[at],
            device_id={"dp": lax.rem(me + n - way(m), n)}, device_id_type=MESH,
        )

    load_g(0).start()
    load_a(0, 0).start()
    barrier = pltpu.get_barrier_semaphore()
    for m in range(RINGS):
        pl.semaphore_signal(barrier, inc=1, device_id={"dp": lax.rem(me + n - way(m), n)}, device_id_type=MESH)
    load_a(0, 0).wait()
    load_g(1).start()
    load_a(1, 0).start()
    load_g(0).wait()
    for k in range(len(STRIPS)):
        strip = STRIPS[k]
        for m in range(RINGS):
            if m == 1 and k == 0:
                load_g(1).wait()
            if k or m:
                load_a(m, k).wait()
            if k + 1 < len(STRIPS):
                load_a(m, k + 1).start()
            else:
                load_g(RINGS + m).start()
                for j in range(len(STRIPS)):
                    load_a(RINGS + m, j).start()
            b = block(m, 0)
            held[m, b, strip[0] : strip[0] + strip[1]] = dot(a_v[m, :, strip[0] : strip[0] + strip[1]], m).astype(held.dtype)
            if m == 0 and k == 0:
                pl.semaphore_wait(barrier, RINGS)
            hop(0, m, 0, b, strip).start()

    def ahead(i):
        @pl.when(i + SLOTS < items)
        def _():
            load_g(i + SLOTS).start()

    ahead(0)
    ahead(1)

    def first(m, c):
        for k in range(len(STRIPS)):
            load_a(m, k).wait()
        load_g(m).wait()
        b = block(m, 0)
        held[m, b] = dot(a_v[m], m).astype(held.dtype)
        hop(0, m, 0, b).start()
        ahead(m)
        return c

    lax.fori_loop(RINGS, matrices, first, 0)

    def term(i):
        load_g(i).wait()
        part[...] = dot(a_v[lax.rem(i, matrices)], i)
        ahead(i)

    def middle(i, c):
        m, s = lax.rem(i, matrices), lax.div(i, matrices)
        term(i)
        b = block(m, s)
        hop(0, m, s - 1, b).wait_recv()
        held[m, b] = (part[...] + held[m, b].astype(jnp.float32)).astype(held.dtype)
        hop(0, m, s, b).start()
        return c

    lax.fori_loop(matrices, items - matrices, middle, 0)

    def last(m, c):
        term(items - matrices + m)
        hop(0, m, n - 2, me).wait_recv()
        out[m, :, tile(me)] = (part[...] + held[m, me].astype(jnp.float32)).astype(out.dtype)
        hop(1, m, 0, me).start()
        return c

    lax.fori_loop(0, matrices, last, 0)

    def gather(i, c):
        m, s = lax.rem(i, matrices), lax.div(i, matrices) + 1
        b = lax.rem(me + n + way(m) * s, n)
        hop(1, m, s - 1, b).wait_recv()

        @pl.when(s < n - 1)
        def _():
            hop(1, m, s, b).start()

        hop(0, m, s - 1, me).wait_send()
        hop(1, m, s - 1, me).wait_send()
        return c

    lax.fori_loop(0, items - matrices, gather, 0)


def write_out(src, dst, sem):
    copies = [pltpu.make_async_copy(src.at[m], dst.at[m], sem.at[m]) for m in range(src.shape[0])]
    for c in copies:
        c.start()
    for c in copies:
        c.wait()


def solution(mesh):
    n = mesh.shape["dp"]

    def step(a, g):
        _, matrices, tokens, d = a.shape
        ff = g.shape[3]
        cols = ff // n
        hops = 2 * n * matrices
        sums = pl.pallas_call(
            functools.partial(kernel, n),
            out_shape=pltpu.VMEM((matrices, d, ff), jnp.bfloat16),
            in_specs=[pl.BlockSpec(memory_space=pl.ANY)] * 2,
            out_specs=pl.BlockSpec(memory_space=pltpu.VMEM),
            scratch_shapes=[
                pltpu.VMEM((matrices, tokens, d), jnp.bfloat16),
                pltpu.VMEM((SLOTS, tokens, cols), jnp.bfloat16),
                pltpu.VMEM((d, cols), jnp.float32),
                pltpu.VMEM((matrices, n, d, cols), jnp.bfloat16),
                pltpu.SemaphoreType.DMA((matrices * len(STRIPS),)),
                pltpu.SemaphoreType.DMA((SLOTS,)),
                pltpu.SemaphoreType.DMA((hops,)),
                pltpu.SemaphoreType.DMA((hops,)),
            ],
            compiler_params=pltpu.CompilerParams(
                collective_id=0, has_side_effects=True, vmem_limit_bytes=49 << 20
            ),
            cost_estimate=pl.CostEstimate(
                flops=2 * matrices * tokens * d * ff, bytes_accessed=2 * matrices * (tokens + d) * (d + ff), transcendentals=0
            ),
        )(a, g)
        return pl.pallas_call(
            write_out,
            out_shape=jax.ShapeDtypeStruct((matrices, d, ff), jnp.bfloat16),
            in_specs=[pl.BlockSpec(memory_space=pltpu.VMEM)],
            out_specs=pl.BlockSpec(memory_space=pl.ANY),
            scratch_shapes=[pltpu.SemaphoreType.DMA((matrices,))],
            compiler_params=pltpu.CompilerParams(has_side_effects=True, vmem_limit_bytes=1 << 20),
        )(sums)

    return jax.shard_map(
        step, mesh=mesh, in_specs=(P(("rep", "dp")), P(("rep", "dp"))), out_specs=P("rep"), check_vma=False
    )
```

```python
import functools

import jax
import jax.numpy as jnp
from jax import lax
from jax.experimental import pallas as pl
from jax.experimental.pallas import tpu as pltpu
from jax.sharding import PartitionSpec as P

MESH = pl.DeviceIdType.MESH
HALVES = 2
SLOTS = 4
STRIP = 128


def kernel(n, a_hbm, g_hbm, out, a_v, g_v, part, held, a_sem, g_sem, send_sem, recv_sem):
    matrices, _, _, rows, cols = held.shape
    me = lax.axis_index("dp")
    peers = (lax.rem(me + 1, n), lax.rem(me + n - 1, n))
    items = n * matrices
    strips = ((0, STRIP), (2 * rows - STRIP, STRIP), (STRIP, 2 * (rows - STRIP)))

    def block(h, s):
        return lax.rem(me + n + n - 1 - s, n) if h == 0 else lax.rem(me + 1 + s, n)

    def tile(h, b):
        return pl.ds(pl.multiple_of((b if h == 0 else lax.rem(b + n - 2, n)) * cols, cols), cols)

    def load_a(m, k=None):
        if k is None:
            return pltpu.make_async_copy(a_hbm.at[0, m], a_v.at[m], a_sem.at[m])
        strip = pl.ds(*strips[k])
        return pltpu.make_async_copy(a_hbm.at[0, m, :, strip], a_v.at[m, :, strip], a_sem.at[k if k == 0 else matrices + k - 1])

    def load_g(i, h):
        slot = lax.rem(2 * i + h, SLOTS)
        return pltpu.make_async_copy(
            g_hbm.at[0, lax.rem(i, matrices), :, tile(h, block(h, lax.div(i, matrices)))], g_v.at[slot], g_sem.at[slot]
        )

    def dot(m, first, size, i, h):
        return lax.dot_general(
            a_v[m, :, first : first + size],
            g_v[lax.rem(2 * i + h, SLOTS)],
            (((0,), (0,)), ((), ())),
            preferred_element_type=jnp.float32,
        )

    def hop(phase, m, h, s, b, strip=None):
        ring = m * HALVES + h
        at = ring * n + lax.rem(s + phase * (n - 1), n)
        if phase:
            ref = out.at[m, pl.ds(h * rows, rows), tile(h, b)]
        else:
            ref = held.at[m, h, b] if strip is None else held.at[m, h, b, pl.ds(*strip)]
        return pltpu.make_async_remote_copy(
            src_ref=ref, dst_ref=ref, send_sem=send_sem.at[ring * 2 + lax.rem(s + phase * (n - 1), 2)], recv_sem=recv_sem.at[at],
            device_id={"dp": peers[h]}, device_id_type=MESH,
        )

    load_g(0, 0).start()
    load_a(0, 0).start()
    load_a(0, 1).start()
    barrier = pltpu.get_barrier_semaphore()
    for p in peers:
        pl.semaphore_signal(barrier, inc=1, device_id={"dp": p}, device_id_type=MESH)
    load_a(0, 0).wait()
    load_a(0, 2).start()
    load_g(0, 0).wait()
    load_g(1, 0).start()
    load_a(1).start()
    for h in range(HALVES):
        b = block(h, 0)
        edge = (0, STRIP) if h == 0 else (rows - STRIP, STRIP)
        if h:
            load_a(0, 1).wait()
        held[0, h, b, edge[0] : edge[0] + STRIP] = dot(0, strips[h][0], STRIP, 0, 0).astype(held.dtype)
        if h == 0:
            pl.semaphore_wait(barrier, len(peers))
        hop(0, 0, h, 0, b, edge).start()
    load_a(0, 2).wait()
    rest = rows - STRIP
    both = dot(0, STRIP, 2 * rest, 0, 0).astype(held.dtype)
    for h in range(HALVES):
        b = block(h, 0)
        edge = (STRIP, rest) if h == 0 else (0, rest)
        held[0, h, b, edge[0] : edge[0] + rest] = both[h * rest : (h + 1) * rest]
        hop(0, 0, h, 0, b, edge).start()

    def first(m, c):
        @pl.when(m + 1 < matrices)
        def _():
            load_g(m + 1, 0).start()
            load_a(m + 1).start()

        load_g(m, 0).wait()
        load_a(m).wait()
        both = dot(m, 0, 2 * rows, m, 0).astype(held.dtype)
        for h in range(HALVES):
            b = block(h, 0)
            held[m, h, b] = both[h * rows : (h + 1) * rows]
            hop(0, m, h, 0, b).start()

        @pl.when(m + 2 >= matrices)
        def _():
            for h in range(HALVES):
                load_g(m + 2, h).start()

        return c

    lax.fori_loop(1, matrices, first, 0)

    def term(i, m, h):
        load_g(i, h).wait()
        part[...] = dot(m, h * rows, rows, i, h)

        @pl.when(i + SLOTS // HALVES < items)
        def _():
            load_g(i + SLOTS // HALVES, h).start()

    def middle(i, c):
        m, s = lax.rem(i, matrices), lax.div(i, matrices)
        for h in range(HALVES):
            term(i, m, h)
            b = block(h, s)
            hop(0, m, h, s - 1, b).wait_recv()
            held[m, h, b] = (part[...] + held[m, h, b].astype(jnp.float32)).astype(held.dtype)

            @pl.when(s >= 2)
            def _():
                hop(0, m, h, s - 2, b).wait_send()

            hop(0, m, h, s, b).start()
        return c

    lax.fori_loop(matrices, items - matrices, middle, 0)

    def last(m, c):
        for h in range(HALVES):
            term(items - matrices + m, m, h)
            hop(0, m, h, n - 2, me).wait_recv()
            out[m, pl.ds(h * rows, rows), tile(h, me)] = (
                part[...] + held[m, h, me].astype(jnp.float32)
            ).astype(out.dtype)
            hop(0, m, h, n - 3, me).wait_send()
            hop(1, m, h, 0, me).start()
        return c

    lax.fori_loop(0, matrices, last, 0)

    def gather(i, c):
        m, s = lax.rem(i, matrices), lax.div(i, matrices) + 1
        for h in range(HALVES):
            b = lax.rem(me + n - s, n) if h == 0 else lax.rem(me + s, n)
            hop(1, m, h, s - 1, b).wait_recv()
            hop(1, m, h, s, b).wait_send()
            hop(1, m, h, s, b).start()
        return c

    lax.fori_loop(0, items - 2 * matrices, gather, 0)

    def end(m, c):
        for h in range(HALVES):
            hop(1, m, h, n - 2, lax.rem(me + 1, n) if h == 0 else lax.rem(me + n - 1, n)).wait_recv()
            for s in range(n - 3, n - 1):
                hop(1, m, h, s, me).wait_send()
        return c

    lax.fori_loop(0, matrices, end, 0)


def write_out(src, dst, sem):
    copies = [pltpu.make_async_copy(src.at[m], dst.at[m], sem.at[m]) for m in range(src.shape[0])]
    for c in copies:
        c.start()
    for c in copies:
        c.wait()


def solution(mesh):
    n = mesh.shape["dp"]

    def step(a, g):
        _, matrices, tokens, d = a.shape
        ff = g.shape[3]
        rows, cols = d // HALVES, ff // n
        rings = matrices * HALVES
        sums = pl.pallas_call(
            functools.partial(kernel, n),
            out_shape=pltpu.VMEM((matrices, d, ff), jnp.bfloat16),
            in_specs=[pl.BlockSpec(memory_space=pl.ANY)] * 2,
            out_specs=pl.BlockSpec(memory_space=pltpu.VMEM),
            scratch_shapes=[
                pltpu.VMEM((matrices, tokens, d), jnp.bfloat16),
                pltpu.VMEM((SLOTS, tokens, cols), jnp.bfloat16),
                pltpu.VMEM((rows, cols), jnp.float32),
                pltpu.VMEM((matrices, HALVES, n, rows, cols), jnp.bfloat16),
                pltpu.SemaphoreType.DMA((matrices + 2,)),
                pltpu.SemaphoreType.DMA((SLOTS,)),
                pltpu.SemaphoreType.DMA((rings * 2,)),
                pltpu.SemaphoreType.DMA((rings * n,)),
            ],
            compiler_params=pltpu.CompilerParams(
                collective_id=0, has_side_effects=True, vmem_limit_bytes=49 << 20
            ),
            cost_estimate=pl.CostEstimate(
                flops=2 * matrices * tokens * d * ff, bytes_accessed=2 * matrices * (tokens + d) * (d + ff), transcendentals=0
            ),
        )(a, g)
        return pl.pallas_call(
            write_out,
            out_shape=jax.ShapeDtypeStruct((matrices, d, ff), jnp.bfloat16),
            in_specs=[pl.BlockSpec(memory_space=pltpu.VMEM)],
            out_specs=pl.BlockSpec(memory_space=pl.ANY),
            scratch_shapes=[pltpu.SemaphoreType.DMA((matrices,))],
            compiler_params=pltpu.CompilerParams(has_side_effects=True, vmem_limit_bytes=1 << 20),
        )(sums)

    return jax.shard_map(
        step, mesh=mesh, in_specs=(P(("rep", "dp")), P(("rep", "dp"))), out_specs=P("rep"), check_vma=False
    )
```

```python
import functools

import jax
import jax.numpy as jnp
from jax import lax
from jax.experimental import pallas as pl
from jax.experimental.pallas import tpu as pltpu
from jax.sharding import PartitionSpec as P

MESH = pl.DeviceIdType.MESH
HALVES = 2
SLOTS = 4
TURNS = 3
STRIP = 128


def kernel(n, a_hbm, g_hbm, out, a_v, g_v, part, held, a_sem, g_sem, send_sem, recv_sem):
    matrices, _, _, rows, cols = held.shape
    me = lax.axis_index("dp")
    peers = (lax.rem(me + 1, n), lax.rem(me + n - 1, n))
    items = n * matrices
    strips = ((0, STRIP), (2 * rows - STRIP, STRIP), (STRIP, 2 * (rows - STRIP)))

    def block(h, s):
        return lax.rem(me + n + n - 1 - s, n) if h == 0 else lax.rem(me + 1 + s, n)

    def tile(h, b):
        return pl.ds(pl.multiple_of((b if h == 0 else lax.rem(b + n - 2, n)) * cols, cols), cols)

    def load_a(m, k=None):
        if k is None:
            return pltpu.make_async_copy(a_hbm.at[0, m], a_v.at[m], a_sem.at[m])
        strip = pl.ds(*strips[k])
        return pltpu.make_async_copy(a_hbm.at[0, m, :, strip], a_v.at[m, :, strip], a_sem.at[k if k == 0 else matrices + k - 1])

    def load_g(i, h):
        slot = lax.rem(2 * i + h, SLOTS)
        return pltpu.make_async_copy(
            g_hbm.at[0, lax.rem(i, matrices), :, tile(h, block(h, lax.div(i, matrices)))], g_v.at[slot], g_sem.at[slot]
        )

    def dot(m, first, size, i, h):
        return lax.dot_general(
            a_v[m, :, first : first + size],
            g_v[lax.rem(2 * i + h, SLOTS)],
            (((0,), (0,)), ((), ())),
            preferred_element_type=jnp.float32,
        )

    def hop(phase, m, h, s, b, strip=None):
        ring, u = m * HALVES + h, s + phase * (n - 1)
        if phase:
            ref = out.at[m, pl.ds(h * rows, rows), tile(h, b)]
        else:
            ref = held.at[m, h, b] if strip is None else held.at[m, h, b, pl.ds(*strip)]
        return pltpu.make_async_remote_copy(
            src_ref=ref, dst_ref=ref, send_sem=send_sem.at[ring], recv_sem=recv_sem.at[ring * TURNS + lax.rem(u, TURNS)],
            device_id={"dp": peers[h]}, device_id_type=MESH,
        )

    load_g(0, 0).start()
    load_a(0, 0).start()
    load_a(0, 1).start()
    barrier = pltpu.get_barrier_semaphore()
    for p in peers:
        pl.semaphore_signal(barrier, inc=1, device_id={"dp": p}, device_id_type=MESH)
    load_a(0, 0).wait()
    load_a(0, 2).start()
    load_g(0, 0).wait()
    load_g(1, 0).start()
    load_a(1).start()
    for h in range(HALVES):
        b = block(h, 0)
        edge = (0, STRIP) if h == 0 else (rows - STRIP, STRIP)
        if h:
            load_a(0, 1).wait()
        held[0, h, b, edge[0] : edge[0] + STRIP] = dot(0, strips[h][0], STRIP, 0, 0).astype(held.dtype)
        if h == 0:
            pl.semaphore_wait(barrier, len(peers))
        hop(0, 0, h, 0, b, edge).start()
    load_a(0, 2).wait()
    rest = rows - STRIP
    both = dot(0, STRIP, 2 * rest, 0, 0).astype(held.dtype)
    for h in range(HALVES):
        b = block(h, 0)
        edge = (STRIP, rest) if h == 0 else (0, rest)
        held[0, h, b, edge[0] : edge[0] + rest] = both[h * rest : (h + 1) * rest]
        hop(0, 0, h, 0, b, edge).start()

    def first(m, c):
        @pl.when(m + 1 < matrices)
        def _():
            load_g(m + 1, 0).start()
            load_a(m + 1).start()

        load_g(m, 0).wait()
        load_a(m).wait()
        both = dot(m, 0, 2 * rows, m, 0).astype(held.dtype)
        for h in range(HALVES):
            b = block(h, 0)
            held[m, h, b] = both[h * rows : (h + 1) * rows]
            hop(0, m, h, 0, b).start()

        @pl.when(m + 2 >= matrices)
        def _():
            for h in range(HALVES):
                load_g(m + 2, h).start()

        return c

    lax.fori_loop(1, matrices, first, 0)

    def term(i, m, h):
        load_g(i, h).wait()
        part[...] = dot(m, h * rows, rows, i, h)

        @pl.when(i + SLOTS // HALVES < items)
        def _():
            load_g(i + SLOTS // HALVES, h).start()

    def middle(i, c):
        m, s = lax.rem(i, matrices), lax.div(i, matrices)
        for h in range(HALVES):
            term(i, m, h)
            b = block(h, s)
            hop(0, m, h, s - 1, b).wait_recv()
            held[m, h, b] = (part[...] + held[m, h, b].astype(jnp.float32)).astype(held.dtype)
            hop(0, m, h, s - 1, b).wait_send()
            hop(0, m, h, s, b).start()
        return c

    lax.fori_loop(matrices, items - matrices, middle, 0)

    def last(m, c):
        for h in range(HALVES):
            term(items - matrices + m, m, h)
            hop(0, m, h, n - 2, me).wait_recv()
            out[m, pl.ds(h * rows, rows), tile(h, me)] = (
                part[...] + held[m, h, me].astype(jnp.float32)
            ).astype(out.dtype)
            hop(0, m, h, n - 2, me).wait_send()
            hop(1, m, h, 0, me).start()
        return c

    lax.fori_loop(0, matrices, last, 0)

    def gather(i, c):
        m, s = lax.rem(i, matrices), lax.div(i, matrices) + 1
        for h in range(HALVES):
            b = lax.rem(me + n - s, n) if h == 0 else lax.rem(me + s, n)
            hop(1, m, h, s - 1, b).wait_recv()
            hop(1, m, h, s - 1, b).wait_send()
            hop(1, m, h, s, b).start()
        return c

    lax.fori_loop(0, items - 2 * matrices, gather, 0)

    def end(m, c):
        for h in range(HALVES):
            hop(1, m, h, n - 2, lax.rem(me + 1, n) if h == 0 else lax.rem(me + n - 1, n)).wait_recv()
            hop(1, m, h, n - 2, me).wait_send()
        return c

    lax.fori_loop(0, matrices, end, 0)


def write_out(src, dst, sem):
    copies = [pltpu.make_async_copy(src.at[m], dst.at[m], sem.at[m]) for m in range(src.shape[0])]
    for c in copies:
        c.start()
    for c in copies:
        c.wait()


def solution(mesh):
    n = mesh.shape["dp"]

    def step(a, g):
        _, matrices, tokens, d = a.shape
        ff = g.shape[3]
        rows, cols = d // HALVES, ff // n
        rings = matrices * HALVES
        sums = pl.pallas_call(
            functools.partial(kernel, n),
            out_shape=pltpu.VMEM((matrices, d, ff), jnp.bfloat16),
            in_specs=[pl.BlockSpec(memory_space=pl.ANY)] * 2,
            out_specs=pl.BlockSpec(memory_space=pltpu.VMEM),
            scratch_shapes=[
                pltpu.VMEM((matrices, tokens, d), jnp.bfloat16),
                pltpu.VMEM((SLOTS, tokens, cols), jnp.bfloat16),
                pltpu.VMEM((rows, cols), jnp.float32),
                pltpu.VMEM((matrices, HALVES, n, rows, cols), jnp.bfloat16),
                pltpu.SemaphoreType.DMA((matrices + 2,)),
                pltpu.SemaphoreType.DMA((SLOTS,)),
                pltpu.SemaphoreType.DMA((rings,)),
                pltpu.SemaphoreType.DMA((rings * TURNS,)),
            ],
            compiler_params=pltpu.CompilerParams(
                collective_id=0, has_side_effects=True, vmem_limit_bytes=49 << 20
            ),
            cost_estimate=pl.CostEstimate(
                flops=2 * matrices * tokens * d * ff, bytes_accessed=2 * matrices * (tokens + d) * (d + ff), transcendentals=0
            ),
        )(a, g)
        return pl.pallas_call(
            write_out,
            out_shape=jax.ShapeDtypeStruct((matrices, d, ff), jnp.bfloat16),
            in_specs=[pl.BlockSpec(memory_space=pltpu.VMEM)],
            out_specs=pl.BlockSpec(memory_space=pl.ANY),
            scratch_shapes=[pltpu.SemaphoreType.DMA((matrices,))],
            compiler_params=pltpu.CompilerParams(has_side_effects=True, vmem_limit_bytes=1 << 20),
        )(sums)

    return jax.shard_map(
        step, mesh=mesh, in_specs=(P(("rep", "dp")), P(("rep", "dp"))), out_specs=P("rep"), check_vma=False
    )
```
